16 devices in a mesh: dp: 4 (over y, z, core), tp: 4 (over x).
Axes of the slice: x: 4, y: 2, z: 1, core: 2. Of those that a mesh axis runs over, the one named last changes fastest.
The devices are a block of a 4x4x8 slice.
Arguments:
- x: bfloat16 [3584, 5120], P(('dp', 'tp')), parts along dimension 0
- w_gate: bfloat16 [5120, 12288], P(None, 'tp')
- w_up: bfloat16 [5120, 12288], P(None, 'tp')
- w_down: bfloat16 [12288, 5120], P('tp')
Outputs:
- output: bfloat16 [3584, 5120], P(('dp', 'tp')), parts along dimension 0
There are 4 independent parts. The reference program is written for one: setup_inputs(seed, part) draws one part's arguments, and reference() takes and returns one part's arrays. A program takes and returns all parts, laid end to end along the dimension named above; an argument that names none is the same for every part.
All inputs are finite; a program needn't handle non-finite values.
Results may differ from the reference program's by a relative error of at most 0.016.
Values are sent between devices in bfloat16 or wider.
A program may use at most 768 MiB of HBM per device.

```python
import jax
import jax.numpy as jnp

ROWS = 896
D = 5120
FF = 12288


def setup_inputs(seed: int = 0, part: int = 0) -> dict:
    kx, kg, ku, kd = jax.random.split(jax.random.key(seed), 4)
    drawn = {
        "x": jax.random.normal(jax.random.fold_in(kx, part), (ROWS, D), jnp.float32),
        "w_gate": jax.random.normal(kg, (D, FF), jnp.float32) * D**-0.5,
        "w_up": jax.random.normal(ku, (D, FF), jnp.float32) * D**-0.5,
        "w_down": jax.random.normal(kd, (FF, D), jnp.float32) * FF**-0.5,
    }
    return {k: v.astype(jnp.bfloat16) for k, v in drawn.items()}


def reference(x, w_gate, w_up, w_down):
    gate = jnp.dot(x, w_gate, preferred_element_type=jnp.float32)
    up = jnp.dot(x, w_up, preferred_element_type=jnp.float32)
    hidden = (jax.nn.silu(gate) * up).astype(jnp.bfloat16)
    return jnp.dot(hidden, w_down, preferred_element_type=jnp.float32).astype(jnp.bfloat16)
```

```python
import functools

import jax
import jax.numpy as jnp
from jax import lax
from jax.experimental import pallas as pl
from jax.experimental.pallas import tpu as pltpu
from jax.sharding import PartitionSpec as P

HALVES = 2
KC = 512
NT = 1536
AHEAD = 3


def when(cond, f):
    if isinstance(cond, bool):
        if cond:
            f()
    else:
        pl.when(cond)(f)


def kernel(
    n, x, wg, wu, wd, y,
    xg, accg, accu, hid, wgu, wdb, pout, pin, qout, qin, tq, own, yst,
    ld_sem, w_sem, wd_sem, own_send, own_recv, fwd_send, fwd_recv,
    p_send, p_recv, q_send, q_recv, y_sem,
):
    me = lax.axis_index("tp")
    right, left = lax.rem(me + 1, n), lax.rem(me + n - 1, n)
    target = (right, left)
    rows, cols = x.shape
    part = rows // HALVES
    chunks = cols // KC
    total = HALVES * chunks
    hidden = wg.shape[1]
    half = KC // 2
    slot = [pl.ds(i * part, part) for i in range(n)]
    side = (pl.ds(0, half), pl.ds(half, half))

    def load(g):
        h, c = g // chunks, g % chunks
        return pltpu.make_async_copy(
            x.at[pl.ds(pl.multiple_of(h * part, part), part), pl.ds(pl.multiple_of(c * KC, KC), KC)],
            xg.at[g, slot[0]],
            ld_sem.at[g],
        )

    def remote(d, src, dst, send, recv):
        return pltpu.make_async_remote_copy(
            src_ref=src, dst_ref=dst, send_sem=send, recv_sem=recv,
            device_id={"tp": target[d]}, device_id_type=pl.DeviceIdType.MESH,
        )

    def own_copy(d, g):
        return remote(d, xg.at[g, slot[0]], xg.at[g, slot[3 if d == 0 else 1]], own_send.at[d, g], own_recv.at[d, g])

    def fwd_copy(d, g):
        cut = side[1 - d]
        return remote(
            d, xg.at[g, slot[3 if d == 0 else 1], cut], xg.at[g, slot[2], cut], fwd_send.at[d, g], fwd_recv.at[d, g]
        )

    def p_copy(d, h, c):
        return remote(d, pout.at[d, c], pin.at[d, h * chunks + c], p_send.at[d, c], p_recv.at[d, h * chunks + c])

    def q_copy(d, h, c):
        return remote(d, qout.at[d, c], qin.at[d, h * chunks + c], q_send.at[d, c], q_recv.at[d, h * chunks + c])

    def w_copies(g):
        s, c = g % 2, g % chunks
        piece = pl.ds(pl.multiple_of(c * KC, KC), KC)
        return [pltpu.make_async_copy(w.at[piece], wgu.at[s, i], w_sem.at[s, i]) for i, w in enumerate((wg, wu))]

    def wd_copy(g):
        s, c = g % 2, g % chunks
        return pltpu.make_async_copy(wd.at[:, pl.ds(pl.multiple_of(c * KC, KC), KC)], wdb.at[s], wd_sem.at[s])

    def y_copy(g):
        h, c = g // chunks, g % chunks
        return pltpu.make_async_copy(
            yst.at[g],
            y.at[pl.ds(pl.multiple_of(h * part, part), part), pl.ds(pl.multiple_of(c * KC, KC), KC)],
            y_sem.at[g],
        )

    def each(count, f):
        def body(i, carry):
            f(i)
            return carry

        lax.fori_loop(0, count, body, 0)

    def start_own(g):
        load(g).wait()
        for d in range(2):
            own_copy(d, g).start()

    def forward(g):
        for d in range(2):
            own_copy(d, g).wait_recv()
            fwd_copy(d, g).start()
        when(g + AHEAD < total, lambda: start_own(g + AHEAD))

    def gate_up(g, first, last):
        s = g % 2
        for copy in w_copies(g):
            copy.wait()

        def tile(j):
            cut = pl.ds(pl.multiple_of(j * NT, NT), NT)
            block = xg[g]
            gate = jnp.dot(block, wgu[s, 0, :, cut], preferred_element_type=jnp.float32)
            if not first:
                gate += accg[:, cut]
            if not last:
                accg[:, cut] = gate
            up = jnp.dot(block, wgu[s, 1, :, cut], preferred_element_type=jnp.float32)
            if not first:
                up += accu[:, cut]
            if not last:
                accu[:, cut] = up
            else:
                hid[:, cut] = (jax.nn.silu(gate) * up).astype(hid.dtype)

        each(hidden // NT, tile)

        def prefetch():
            for copy in w_copies(g + 2):
                copy.start()

        when(g + 2 < total, prefetch)

    def gather_phase(h, before):
        def step(c, first, last):
            g = h * chunks + c
            before(c)
            for d in range(2):
                fwd_copy(d, g).wait_recv()
            gate_up(g, first, last)

        step(0, True, False)
        each(chunks - 2, lambda i: step(i + 1, False, False))
        step(chunks - 1, False, True)

    def down(h, c):
        g = h * chunks + c
        s = g % 2
        wd_copy(g).wait()
        if h:
            for d in range(2):
                p_copy(d, h - 1, c).wait_send()
        term = jnp.dot(hid[...], wdb[s], preferred_element_type=jnp.float32)
        mine = [term[i * part : (i + 1) * part] for i in range(n)]
        for d in range(2):
            near = mine[1 if d == 0 else 3]
            lo = slice(d * half, (d + 1) * half)
            hi = slice((1 - d) * half, (2 - d) * half)
            pout[d, c, 0] = mine[2][:, lo].astype(pout.dtype)
            pout[d, c, 1] = near[:, hi].astype(pout.dtype)
            tq[d, c] = near[:, lo]
        own[g] = mine[0]
        when(g + 2 < total, lambda: wd_copy(g + 2).start())

    def send_p(h, c):
        for d in range(2):
            p_copy(d, h, c).start()

    def sum_q(h, c):
        g = h * chunks + c
        for d in range(2):
            p_copy(d, h, c).wait_recv()
            if h:
                q_copy(d, h - 1, c).wait_send()
            qout[d, c] = (tq[d, c] + pin[d, g, 0].astype(jnp.float32)).astype(qout.dtype)

    def send_q(h, c):
        for d in range(2):
            q_copy(d, h, c).start()

    def finish(h, c):
        g = h * chunks + c
        for d in range(2):
            q_copy(d, h, c).wait_recv()
        for d in range(2):
            cut = side[d]
            out = own[g, :, cut] + qin[d, g].astype(jnp.float32) + pin[1 - d, g, 1].astype(jnp.float32)
            yst[g, :, cut] = out.astype(yst.dtype)
        y_copy(g).start()

    load(0).start()
    for copy in w_copies(0):
        copy.start()
    each(total - 1, lambda i: load(i + 1).start())
    for copy in w_copies(1):
        copy.start()
    for g in range(2):
        wd_copy(g).start()
    barrier = pltpu.get_barrier_semaphore()
    for neighbour in target:
        pl.semaphore_signal(barrier, inc=1, device_id={"tp": neighbour}, device_id_type=pl.DeviceIdType.MESH)
    pl.semaphore_wait(barrier, 2)

    for g in range(AHEAD):
        start_own(g)
    forward(0)

    gather_phase(0, lambda c: forward(c + 1))

    def down0(c):
        when(c % 2 == 0, lambda: forward(chunks + 1 + c // 2))
        down(0, c)

    each(chunks, down0)

    passed = chunks + 1 + (chunks + 1) // 2

    def before1(c):
        when(passed + c < total, lambda: forward(passed + c))
        for k in range(2):
            i = 2 * (c - 2) + k
            when((i >= 0) & (i < chunks) if not isinstance(i, int) else 0 <= i < chunks, lambda i=i: send_p(0, i))
        for k in range(2):
            i = 2 * (c - 7) + k
            ok = (i >= 0) & (i < chunks) if not isinstance(i, int) else 0 <= i < chunks

            def pair(i=i):
                sum_q(0, i)
                send_q(0, i)

            when(ok, pair)

    gather_phase(1, before1)

    summed = 2 * (chunks - 7)

    def down1(c):
        when(summed + c < chunks, lambda: sum_q(0, summed + c))
        down(1, c)
        when(summed + c < chunks, lambda: send_q(0, summed + c))
        send_p(1, c)

    each(chunks, down1)

    def tail(c):
        sum_q(1, c)
        finish(0, c)
        send_q(1, c)

    each(chunks, tail)
    each(chunks, lambda c: finish(1, c))

    def drain(g):
        for d in range(2):
            own_copy(d, g).wait_send()
            fwd_copy(d, g).wait_send()
        y_copy(g).wait()

    each(total, drain)

    def drain_sums(c):
        for d in range(2):
            p_copy(d, 1, c).wait_send()
            q_copy(d, 1, c).wait_send()

    each(chunks, drain_sums)


def solution(mesh):
    n = mesh.shape["tp"]

    def step(x, w_gate, w_up, w_down):
        rows, cols = x.shape
        hidden = w_gate.shape[1]
        part = rows // HALVES
        chunks = cols // KC
        total = HALVES * chunks
        half = KC // 2
        assert n == 4 and rows % HALVES == 0 and cols % KC == 0 and chunks % 2 == 0
        f32, b16 = jnp.float32, x.dtype
        return pl.pallas_call(
            functools.partial(kernel, n),
            out_shape=jax.ShapeDtypeStruct((rows, cols), b16),
            in_specs=[pl.BlockSpec(memory_space=pl.ANY)] * 4,
            out_specs=pl.BlockSpec(memory_space=pl.ANY),
            scratch_shapes=[
                pltpu.VMEM((total, n * part, KC), b16),
                pltpu.VMEM((n * part, hidden), f32),
                pltpu.VMEM((n * part, hidden), f32),
                pltpu.VMEM((n * part, hidden), b16),
                pltpu.VMEM((2, 2, KC, hidden), b16),
                pltpu.VMEM((2, hidden, KC), b16),
                pltpu.VMEM((2, chunks, 2, part, half), b16),
                pltpu.VMEM((2, total, 2, part, half), b16),
                pltpu.VMEM((2, chunks, part, half), b16),
                pltpu.VMEM((2, total, part, half), b16),
                pltpu.VMEM((2, chunks, part, half), f32),
                pltpu.VMEM((total, part, KC), f32),
                pltpu.VMEM((total, part, KC), b16),
                pltpu.SemaphoreType.DMA((total,)),
                pltpu.SemaphoreType.DMA((2, 2)),
                pltpu.SemaphoreType.DMA((2,)),
                pltpu.SemaphoreType.DMA((2, total)),
                pltpu.SemaphoreType.DMA((2, total)),
                pltpu.SemaphoreType.DMA((2, total)),
                pltpu.SemaphoreType.DMA((2, total)),
                pltpu.SemaphoreType.DMA((2, chunks)),
                pltpu.SemaphoreType.DMA((2, total)),
                pltpu.SemaphoreType.DMA((2, chunks)),
                pltpu.SemaphoreType.DMA((2, total)),
                pltpu.SemaphoreType.DMA((total,)),
            ],
            compiler_params=pltpu.CompilerParams(
                collective_id=0, has_side_effects=True, vmem_limit_bytes=67043328
            ),
            name="mlp_ring",
        )(x, w_gate, w_up, w_down)

    return jax.shard_map(
        step,
        mesh=mesh,
        in_specs=(P(("dp", "tp"), None), P(None, "tp"), P(None, "tp"), P("tp", None)),
        out_specs=P(("dp", "tp"), None),
        check_vma=False,
    )
```

```python
import functools

import jax
import jax.numpy as jnp
from jax import lax
from jax.experimental import pallas as pl
from jax.experimental.pallas import tpu as pltpu
from jax.sharding import PartitionSpec as P

HALVES = 2
KC = 1024
KT = KC // 2
NT = 1536
AHEAD = 2
PLAN = (
    {(0, 0): [("f", 1)], (0, 1): [("f", 2)], (2, 0): [("f", 3)], (3, 0): [("f", 4)], (4, 0): [("f", 5)]},
    {(0, 0): [("f", 6)], (1, 1): [("p", 0)], (3, 0): [("f", 7)]},
    {(0, 0): [("p", 1), ("q", 0)], (1, 0): [("f", 8)], (1, 1): [("p", 2)], (2, 0): [("f", 9)], (2, 1): [("p", 3)], (3, 0): [("q", 1)], (3, 1): [("p", 4), ("q", 2)]},
    {(0, 0): [("q", 3)], (0, 1): [("q", 4)]},
)


def when(cond, f):
    if isinstance(cond, bool):
        if cond:
            f()
    else:
        pl.when(cond)(f)


def kernel(
    n, x, wg, wu, wd, y,
    xg, accg, accu, hid, wgu, wdb, pout, pin, qout, qin, tq, own,
    ld_sem, w_sem, wd_sem, own_send, own_recv, fwd_send, fwd_recv,
    p_send, p_recv, q_send, q_recv,
):
    me = lax.axis_index("tp")
    right, left = lax.rem(me + 1, n), lax.rem(me + n - 1, n)
    target = (right, left)
    rows, cols = x.shape
    part = rows // HALVES
    chunks = cols // KC
    total = HALVES * chunks
    hidden = wg.shape[1]
    half = KC // 2
    slot = [pl.ds(i * part, part) for i in range(n)]
    side = (pl.ds(0, half), pl.ds(half, half))

    def load(g):
        h, c = g // chunks, g % chunks
        return pltpu.make_async_copy(
            x.at[pl.ds(pl.multiple_of(h * part, part), part), pl.ds(pl.multiple_of(c * KC, KC), KC)],
            xg.at[g, slot[0]],
            ld_sem.at[g],
        )

    def remote(d, src, dst, send, recv):
        return pltpu.make_async_remote_copy(
            src_ref=src, dst_ref=dst, send_sem=send, recv_sem=recv,
            device_id={"tp": target[d]}, device_id_type=pl.DeviceIdType.MESH,
        )

    def own_copy(d, g):
        return remote(d, xg.at[g, slot[0]], xg.at[g, slot[3 if d == 0 else 1]], own_send.at[d, g], own_recv.at[d, g])

    def fwd_copy(d, g):
        cut = side[1 - d]
        return remote(
            d, xg.at[g, slot[3 if d == 0 else 1], cut], xg.at[g, slot[2], cut], fwd_send.at[d, g], fwd_recv.at[d, g]
        )

    def p_copy(d, h, c):
        return remote(d, pout.at[d, c], pin.at[d, h * chunks + c], p_send.at[d, c], p_recv.at[d, h * chunks + c])

    def q_copy(d, h, c):
        return remote(d, qout.at[d, c], qin.at[d, h * chunks + c], q_send.at[d, c], q_recv.at[d, h * chunks + c])

    tiles = 2 * chunks

    wide = hidden // 2

    def w_copies(g, s):
        piece = pl.ds(pl.multiple_of(g % chunks * KC, KC), KC), pl.ds(s * wide, wide)
        return [pltpu.make_async_copy(w.at[piece], wgu.at[s, k], w_sem.at[s, k]) for k, w in enumerate((wg, wu))]

    def wd_copy(i):
        s, piece = i % 2, pl.ds(pl.multiple_of(i % tiles * KT, KT), KT)
        return pltpu.make_async_copy(wd.at[:, piece], wdb.at[s], wd_sem.at[s])

    def each(count, f):
        def body(i, carry):
            f(i)
            return carry

        lax.fori_loop(0, count, body, 0)

    def start_own(g):
        load(g).wait()
        for d in range(2):
            own_copy(d, g).start()

    def forward(g):
        for d in range(2):
            own_copy(d, g).wait_recv()
            fwd_copy(d, g).start()
        when(g + AHEAD < total, lambda: start_own(g + AHEAD))

    def gate_up(g, s, first, last):
        for copy in w_copies(g, s):
            copy.wait()

        def tile(j):
            w_cut = pl.ds(pl.multiple_of(j * NT, NT), NT)
            cut = pl.ds(pl.multiple_of(s * wide + j * NT, NT), NT)
            block = xg[g]
            gate = jnp.dot(block, wgu[s, 0, :, w_cut], preferred_element_type=jnp.float32)
            if not first:
                gate += accg[:, cut]
            if not last:
                accg[:, cut] = gate
            up = jnp.dot(block, wgu[s, 1, :, w_cut], preferred_element_type=jnp.float32)
            if not first:
                up += accu[:, cut]
            if not last:
                accu[:, cut] = up
            else:
                hid[:, cut] = (jax.nn.silu(gate) * up).astype(hid.dtype)

        each(wide // NT, tile)

        def prefetch():
            for copy in w_copies(g + 1, s):
                copy.start()

        when(g + 1 < total, prefetch)

    def gather_phase(h, before):
        def step(c, first, last):
            g = h * chunks + c
            before(c, 0)
            for d in range(2):
                fwd_copy(d, g).wait_recv()
            gate_up(g, 0, first, last)
            before(c, 1)
            gate_up(g, 1, first, last)

        step(0, True, False)
        each(chunks - 2, lambda i: step(i + 1, False, False))
        step(chunks - 1, False, True)

    def down(h, c, before):
        g = h * chunks + c
        if h:
            for d in range(2):
                p_copy(d, h - 1, c).wait_send()
        for s in range(2):
            before(c, s)
            i = 2 * g + s
            wd_copy(i).wait()
            term = jnp.dot(hid[...], wdb[s], preferred_element_type=jnp.float32)
            mine, near, far, last = [term[k * part : (k + 1) * part] for k in range(n)]
            if s:
                near, last = last, near
            pout[s, c, 0] = far.astype(pout.dtype)
            tq[s, c] = near
            pout[1 - s, c, 1] = last.astype(pout.dtype)
            own[g, :, side[s]] = mine
            when(i + 2 < 2 * total, lambda: wd_copy(i + 2).start())

    def send_p(h, c):
        for d in range(2):
            p_copy(d, h, c).start()

    def sum_q(h, c):
        g = h * chunks + c
        for d in range(2):
            p_copy(d, h, c).wait_recv()
            if h:
                q_copy(d, h - 1, c).wait_send()
            qout[d, c] = (tq[d, c] + pin[d, g, 0].astype(jnp.float32)).astype(qout.dtype)
        for d in range(2):
            own[g, :, side[d]] += pin[1 - d, g, 1].astype(jnp.float32)

    def send_q(h, c):
        for d in range(2):
            q_copy(d, h, c).start()

    def finish(h, c):
        g = h * chunks + c
        for d in range(2):
            q_copy(d, h, c).wait_recv()
            y[
                pl.ds(pl.multiple_of(h * part, part), part), pl.ds(pl.multiple_of(c * KC + d * half, half), half)
            ] = (own[g, :, side[d]] + qin[d, g].astype(jnp.float32)).astype(y.dtype)

    barrier = pltpu.get_barrier_semaphore()
    for neighbour in target:
        pl.semaphore_signal(barrier, inc=1, device_id={"tp": neighbour}, device_id_type=pl.DeviceIdType.MESH)
    for g in range(AHEAD):
        load(g).start()
    pl.semaphore_wait(barrier, 2)
    for g in range(AHEAD):
        start_own(g)
    for s in range(2):
        for copy in w_copies(0, s):
            copy.start()
    each(total - AHEAD, lambda i: load(i + AHEAD).start())
    for i in range(2):
        wd_copy(i).start()
    forward(0)

    def send_sum(c):
        sum_q(0, c)
        send_q(0, c)

    acts = {"f": forward, "p": lambda c: send_p(0, c), "q": send_sum}

    def slots(phase):
        def before(c, s):
            for (k, t), todo in PLAN[phase].items():
                if t == s and (not isinstance(c, int) or c == k):

                    def go(todo=todo):
                        for name, i in todo:
                            acts[name](i)

                    when(c == k, go)

        return before

    gather_phase(0, slots(0))
    each(chunks, lambda c: down(0, c, slots(1)))
    gather_phase(1, slots(2))

    def down1(c):
        down(1, c, slots(3))
        send_p(1, c)

    each(chunks, down1)

    def tail(c):
        sum_q(1, c)
        finish(0, c)
        send_q(1, c)

    each(chunks, tail)

    def drain(g):
        for d in range(2):
            own_copy(d, g).wait_send()
            fwd_copy(d, g).wait_send()

    each(total, drain)

    def drain_sums(c):
        for d in range(2):
            p_copy(d, 1, c).wait_send()

    each(chunks, drain_sums)

    def end(c):
        finish(1, c)
        for d in range(2):
            q_copy(d, 1, c).wait_send()

    each(chunks, end)


def solution(mesh):
    n = mesh.shape["tp"]

    def step(x, w_gate, w_up, w_down):
        rows, cols = x.shape
        hidden = w_gate.shape[1]
        part = rows // HALVES
        chunks = cols // KC
        total = HALVES * chunks
        half = KC // 2
        assert n == 4 and HALVES == 2 and rows % HALVES == 0 and cols % KC == 0 and 2 * chunks == 1 + sum(k == "f" for p in PLAN for todo in p.values() for k, _ in todo)
        f32, b16 = jnp.float32, x.dtype
        return pl.pallas_call(
            functools.partial(kernel, n),
            out_shape=pltpu.VMEM((rows, cols), b16),
            in_specs=[pl.BlockSpec(memory_space=pl.ANY)] * 4,
            out_specs=pl.BlockSpec(memory_space=pltpu.VMEM),
            scratch_shapes=[
                pltpu.VMEM((total, n * part, KC), b16),
                pltpu.VMEM((n * part, hidden), f32),
                pltpu.VMEM((n * part, hidden), f32),
                pltpu.VMEM((n * part, hidden), b16),
                pltpu.VMEM((2, 2, KC, hidden // 2), b16),
                pltpu.VMEM((2, hidden, KT), b16),
                pltpu.VMEM((2, chunks, 2, part, half), b16),
                pltpu.VMEM((2, total, 2, part, half), b16),
                pltpu.VMEM((2, chunks, part, half), b16),
                pltpu.VMEM((2, total, part, half), b16),
                pltpu.VMEM((2, chunks, part, half), f32),
                pltpu.VMEM((total, part, KC), f32),
                pltpu.SemaphoreType.DMA((total,)),
                pltpu.SemaphoreType.DMA((2, 2)),
                pltpu.SemaphoreType.DMA((2,)),
                pltpu.SemaphoreType.DMA((2, total)),
                pltpu.SemaphoreType.DMA((2, total)),
                pltpu.SemaphoreType.DMA((2, total)),
                pltpu.SemaphoreType.DMA((2, total)),
                pltpu.SemaphoreType.DMA((2, chunks)),
                pltpu.SemaphoreType.DMA((2, total)),
                pltpu.SemaphoreType.DMA((2, chunks)),
                pltpu.SemaphoreType.DMA((2, total)),
            ],
            compiler_params=pltpu.CompilerParams(
                collective_id=0, has_side_effects=True, vmem_limit_bytes=64_700_000
            ),
            name="mlp_ring",
        )(x, w_gate, w_up, w_down)

    return jax.shard_map(
        step,
        mesh=mesh,
        in_specs=(P(("dp", "tp"), None), P(None, "tp"), P(None, "tp"), P("tp", None)),
        out_specs=P(("dp", "tp"), None),
        check_vma=False,
    )
```

```python
import functools

import jax
import jax.numpy as jnp
from jax import lax
from jax.experimental import pallas as pl
from jax.experimental.pallas import tpu as pltpu
from jax.sharding import PartitionSpec as P

HALVES = 2
KC = 1024
KT = KC // 2
NT = 1536
GATHER = ((0, 1), (1, 1), (2, 1), (3, 1), (4, 1), (5, 2), (7, 3))
SUMS = (((0, 2), (2, 3)), ((0, 1), (1, 1), (2, 1), (3, 1), (4, 1)))
AHEAD = 2
PLAN = (
    {(0, 0): [("o", 2), ("f", 1)], (0, 1): [("o", 3), ("f", 2)], (1, 0): [("o", 4)], (2, 0): [("f", 3)], (2, 1): [("f", 4), ("o", 5), ("o", 6)]},
    {(0, 1): [("f", 5)], (3, 1): [("f", 6)], (4, 1): [("p", 0)]},
    {(0, 1): [("p", 1)], (3, 0): [("q", 0)], (4, 1): [("q", 1)]},
    {},
)


def when(cond, f):
    if isinstance(cond, bool):
        if cond:
            f()
    else:
        pl.when(cond)(f)


def kernel(
    n, x, wg, wu, wd, y,
    xg, accg, accu, hid, wgu, wdb, pout, pin, qout, qin, tq, own,
    ld_sem, w_sem, wd_sem, own_send, own_recv, fwd_send, fwd_recv,
    p_send, p_recv, q_send, q_recv,
):
    me = lax.axis_index("tp")
    right, left = lax.rem(me + 1, n), lax.rem(me + n - 1, n)
    target = (right, left)
    rows, cols = x.shape
    part = rows // HALVES
    chunks = cols // KC
    total = HALVES * chunks
    hidden = wg.shape[1]
    half = KC // 2
    slot = [pl.ds(i * part, part) for i in range(n)]
    side = (pl.ds(0, half), pl.ds(half, half))

    def load(g):
        h, c = g // chunks, g % chunks
        return pltpu.make_async_copy(
            x.at[pl.ds(pl.multiple_of(h * part, part), part), pl.ds(pl.multiple_of(c * KC, KC), KC)],
            xg.at[g, slot[0]],
            ld_sem.at[g],
        )

    def remote(d, src, dst, send, recv):
        return pltpu.make_async_remote_copy(
            src_ref=src, dst_ref=dst, send_sem=send, recv_sem=recv,
            device_id={"tp": target[d]}, device_id_type=pl.DeviceIdType.MESH,
        )

    def own_copy(d, j):
        a = pl.ds(*GATHER[j])
        src = x.at[slot[0], pl.ds(0, KC)] if j == 0 else xg.at[a, slot[0]]
        dst = xg.at[0 if j == 0 else a, slot[3 if d == 0 else 1]]
        return remote(d, src, dst, own_send.at[d, j], own_recv.at[d, j])

    def fwd_copy(d, j):
        a, cut = pl.ds(*GATHER[j]), side[1 - d]
        return remote(
            d, xg.at[a, slot[3 if d == 0 else 1], cut], xg.at[a, slot[2], cut], fwd_send.at[d, j], fwd_recv.at[d, j]
        )

    def sum_copy(d, h, j, src, dst, send, recv):
        a, k = SUMS[h][j]
        t = j + h * len(SUMS[0])
        return remote(
            d, src.at[d, pl.ds(a, k)], dst.at[d, pl.ds(h * chunks + a, k)], send.at[d, t], recv.at[d, t]
        )

    def p_copy(d, h, j):
        return sum_copy(d, h, j, pout, pin, p_send, p_recv)

    def q_copy(d, h, j):
        return sum_copy(d, h, j, qout, qin, q_send, q_recv)

    def both(f):
        for d in range(2):
            f(d)

    def at_first(groups, c, f):
        for j, (a, _) in enumerate(groups):
            when(c == a, lambda j=j: f(j))

    def at_last(groups, c, f):
        for j, (a, k) in enumerate(groups):
            when(c == a + k - 1, lambda j=j: f(j))

    tiles = 2 * chunks

    wide = hidden // 2

    def w_copies(g, s):
        piece = pl.ds(pl.multiple_of(g % chunks * KC, KC), KC), pl.ds(s * wide, wide)
        return [pltpu.make_async_copy(w.at[piece], wgu.at[s, k], w_sem.at[s, k]) for k, w in enumerate((wg, wu))]

    def wd_copy(i):
        s, piece = i % 2, pl.ds(pl.multiple_of(i % tiles * KT, KT), KT)
        return pltpu.make_async_copy(wd.at[:, piece], wdb.at[s], wd_sem.at[s])

    def each(count, f):
        def body(i, carry):
            f(i)
            return carry

        lax.fori_loop(0, count, body, 0)

    def start_own(j):
        a, k = GATHER[j]
        if j:
            for g in range(a, a + k):
                load(g).wait()
        both(lambda d: own_copy(d, j).start())

    def forward(j):
        for d in range(2):
            own_copy(d, j).wait_recv()
            fwd_copy(d, j).start()

    def gate_up(g, s, first, last):
        for copy in w_copies(g, s):
            copy.wait()

        def tile(j):
            w_cut = pl.ds(pl.multiple_of(j * NT, NT), NT)
            cut = pl.ds(pl.multiple_of(s * wide + j * NT, NT), NT)
            block = xg[g]
            gate = jnp.dot(block, wgu[s, 0, :, w_cut], preferred_element_type=jnp.float32)
            if not first:
                gate += accg[:, cut]
            if not last:
                accg[:, cut] = gate
            up = jnp.dot(block, wgu[s, 1, :, w_cut], preferred_element_type=jnp.float32)
            if not first:
                up += accu[:, cut]
            if not last:
                accu[:, cut] = up
            else:
                hid[:, cut] = (jax.nn.silu(gate) * up).astype(hid.dtype)

        each(wide // NT, tile)

        def prefetch():
            for copy in w_copies(g + 1, s):
                copy.start()

        when(g + 1 < total, prefetch)

    def gather_phase(h, before):
        def step(c, first, last):
            g = h * chunks + c
            before(c, 0)
            for j, (a, _) in enumerate(GATHER):
                if a // chunks == h:
                    when(c == a - h * chunks, lambda j=j: both(lambda d: fwd_copy(d, j).wait_recv()))
            gate_up(g, 0, first, last)
            before(c, 1)
            gate_up(g, 1, first, last)

        step(0, True, False)
        each(chunks - 2, lambda i: step(i + 1, False, False))
        step(chunks - 1, False, True)

    def down(h, c, before):
        g = h * chunks + c
        if h:
            at_first(SUMS[0], c, lambda j: both(lambda d: p_copy(d, 0, j).wait_send()))
        for s in range(2):
            before(c, s)
            i = 2 * g + s
            wd_copy(i).wait()
            term = jnp.dot(hid[...], wdb[s], preferred_element_type=jnp.float32)
            mine, near, far, last = [term[k * part : (k + 1) * part] for k in range(n)]
            if s:
                near, last = last, near
            pout[s, c, 0] = far.astype(pout.dtype)
            tq[s, c] = near
            pout[1 - s, c, 1] = last.astype(pout.dtype)
            own[g, :, side[s]] = mine
            when(i + 2 < 2 * total, lambda: wd_copy(i + 2).start())

    def add(h, c):
        g = h * chunks + c
        for d in range(2):
            qout[d, c] = (tq[d, c] + pin[d, g, 0].astype(jnp.float32)).astype(qout.dtype)
        for d in range(2):
            own[g, :, side[d]] += pin[1 - d, g, 1].astype(jnp.float32)

    def finish(h, c):
        g = h * chunks + c
        for d in range(2):
            y[
                pl.ds(pl.multiple_of(h * part, part), part), pl.ds(pl.multiple_of(c * KC + d * half, half), half)
            ] = (own[g, :, side[d]] + qin[d, g].astype(jnp.float32)).astype(y.dtype)

    barrier = pltpu.get_barrier_semaphore()
    for neighbour in target:
        pl.semaphore_signal(barrier, inc=1, device_id={"tp": neighbour}, device_id_type=pl.DeviceIdType.MESH)
    for g in range(AHEAD):
        load(g).start()
    pl.semaphore_wait(barrier, 2)
    for j in range(AHEAD):
        start_own(j)
    for s in range(2):
        for copy in w_copies(0, s):
            copy.start()
    each(total - AHEAD, lambda i: load(i + AHEAD).start())
    for i in range(2):
        wd_copy(i).start()
    load(0).wait()
    forward(0)

    def send_terms(j):
        both(lambda d: p_copy(d, 0, j).start())

    def send_sums(j):
        a, k = SUMS[0][j]
        both(lambda d: p_copy(d, 0, j).wait_recv())
        each(k, lambda i: add(0, a + i))
        both(lambda d: q_copy(d, 0, j).start())

    acts = {"o": start_own, "f": forward, "p": send_terms, "q": send_sums}

    def slots(phase):
        def before(c, s):
            for (k, t), todo in PLAN[phase].items():
                if t == s and (not isinstance(c, int) or c == k):

                    def go(todo=todo):
                        for name, j in todo:
                            acts[name](j)

                    when(c == k, go)

        return before

    gather_phase(0, slots(0))
    each(chunks, lambda c: down(0, c, slots(1)))
    gather_phase(1, slots(2))

    def down1(c):
        down(1, c, slots(3))
        at_last(SUMS[1], c, lambda j: both(lambda d: p_copy(d, 1, j).start()))

    each(chunks, down1)

    def tail(c):
        at_first(SUMS[1], c, lambda j: both(lambda d: p_copy(d, 1, j).wait_recv()))
        at_first(SUMS[0], c, lambda j: both(lambda d: q_copy(d, 0, j).wait()))
        add(1, c)
        finish(0, c)
        at_last(SUMS[1], c, lambda j: both(lambda d: q_copy(d, 1, j).start()))

    each(chunks, tail)
    for d in range(2):
        for j in range(len(GATHER)):
            own_copy(d, j).wait_send()
            fwd_copy(d, j).wait_send()
        for j in range(len(SUMS[1])):
            p_copy(d, 1, j).wait_send()

    def end(c):
        at_first(SUMS[1], c, lambda j: both(lambda d: q_copy(d, 1, j).wait()))
        finish(1, c)

    each(chunks, end)


def solution(mesh):
    n = mesh.shape["tp"]

    def step(x, w_gate, w_up, w_down):
        rows, cols = x.shape
        hidden = w_gate.shape[1]
        part = rows // HALVES
        chunks = cols // KC
        total = HALVES * chunks
        half = KC // 2
        assert n == 4 and rows % HALVES == 0 and cols % KC == 0
        assert GATHER[0] == (0, 1) and GATHER[AHEAD - 1][0] < chunks and sum(k for _, k in GATHER) == total
        assert len(SUMS) == HALVES and all(sum(k for _, k in groups) == chunks for groups in SUMS)
        sums = sum(len(groups) for groups in SUMS)
        f32, b16 = jnp.float32, x.dtype
        return pl.pallas_call(
            functools.partial(kernel, n),
            out_shape=pltpu.VMEM((rows, cols), b16),
            in_specs=[pl.BlockSpec(memory_space=pl.ANY)] * 4,
            out_specs=pl.BlockSpec(memory_space=pltpu.VMEM),
            scratch_shapes=[
                pltpu.VMEM((total, n * part, KC), b16),
                pltpu.VMEM((n * part, hidden), f32),
                pltpu.VMEM((n * part, hidden), f32),
                pltpu.VMEM((n * part, hidden), b16),
                pltpu.VMEM((2, 2, KC, hidden // 2), b16),
                pltpu.VMEM((2, hidden, KT), b16),
                pltpu.VMEM((2, chunks, 2, part, half), b16),
                pltpu.VMEM((2, total, 2, part, half), b16),
                pltpu.VMEM((2, chunks, part, half), b16),
                pltpu.VMEM((2, total, part, half), b16),
                pltpu.VMEM((2, chunks, part, half), f32),
                pltpu.VMEM((total, part, KC), f32),
                pltpu.SemaphoreType.DMA((total,)),
                pltpu.SemaphoreType.DMA((2, 2)),
                pltpu.SemaphoreType.DMA((2,)),
                pltpu.SemaphoreType.DMA((2, len(GATHER))),
                pltpu.SemaphoreType.DMA((2, len(GATHER))),
                pltpu.SemaphoreType.DMA((2, len(GATHER))),
                pltpu.SemaphoreType.DMA((2, len(GATHER))),
                pltpu.SemaphoreType.DMA((2, sums)),
                pltpu.SemaphoreType.DMA((2, sums)),
                pltpu.SemaphoreType.DMA((2, sums)),
                pltpu.SemaphoreType.DMA((2, sums)),
            ],
            compiler_params=pltpu.CompilerParams(
                collective_id=0, has_side_effects=True, vmem_limit_bytes=64_700_000
            ),
            name="mlp_ring",
        )(x, w_gate, w_up, w_down)

    return jax.shard_map(
        step,
        mesh=mesh,
        in_specs=(P(("dp", "tp"), None), P(None, "tp"), P(None, "tp"), P("tp", None)),
        out_specs=P(("dp", "tp"), None),
        check_vma=False,
    )
```
